32 devices in a mesh: group: 4 (over y, core), dev: 8 (over z, x).
Axes of the slice: x: 2, y: 2, z: 4, core: 2. Of those that a mesh axis runs over, the one named last changes fastest.
Arguments:
- solution: float32 [4, 16, 16, 512], P('group', 'dev'), may hold values from -6 to 6
- residual: float32 [4, 16, 16, 512], P('group', 'dev'), may hold values from -6 to 6
- direction: float32 [4, 16, 16, 512], P('group', 'dev'), may hold values from -0.03 to 0.03
- geometry: bfloat16 [3, 4, 16, 16, 512], P(None, 'group', 'dev'), may hold values from 0.5 to 2
- mass: bfloat16 [4, 16, 16, 512], P('group', 'dev'), may hold values from 50 to 500
Outputs:
- solution_out: float32 [4, 16, 16, 512], P('group', 'dev')
- residual_out: float32 [4, 16, 16, 512], P('group', 'dev')
- direction_out: float32 [4, 16, 16, 512], P('group', 'dev')
The draws below stay inside these ranges and needn't reach their ends.
All inputs are finite; a program needn't handle non-finite values.
Results may differ from the reference program's by a relative error of at most 0.0003.
Values sent between devices are 32-bit elements; how exact they have to be, the bound alone decides.
A program may use at most 64 MiB of HBM per device.

```python
import math
import jax
import jax.numpy as jnp
import numpy as np
from jax import lax

NP = 8
EZ = 16
EA = 4
EB = 16


def draw_direction(key, part):
    position = jnp.arange(EA, dtype=jnp.float32) / max(EA - 1, 1)
    shape = (EA, EB, EZ, NP ** 3)
    noise = jnp.clip(jax.random.normal(key, shape, jnp.float32), -6.0, 6.0)
    rise = jnp.power(4.0, position)
    return (0.001 * rise[:, None, None, None] * noise).astype(jnp.float32)


def level_of(stream_key, dims, split, least, largest):
    factor_of, own = 1.0, jax.random.fold_in(stream_key, 6)
    for dim, parts in split:
        steps = jnp.exp(jax.random.uniform(jax.random.fold_in(own, dim), (parts,), jnp.float32, least / len(split), largest / len(split)))
        factor_of = factor_of * jnp.repeat(steps, dims[dim] // parts).reshape([-1 if axis == dim else 1 for axis in range(len(dims))])
    return factor_of


def centred(key, dims, deviation, limit, shards=(), kind=jnp.bfloat16):
    entries = deviation * jax.random.normal(key, dims, jnp.float32)
    if shards:
        entries = entries * level_of(key, dims, shards, -0.22, 0.18)
    return jnp.clip(entries, -limit, limit).astype(kind)


def setup_inputs(seed: int = 0) -> dict:
    splits = jax.random.split(jax.random.key(seed), 6)
    solution = centred(splits[0], (EA, EB, EZ, NP ** 3), 1.0, 6.0, ((0, 4), (1, 8)), jnp.float32)
    residual = centred(splits[1], (EA, EB, EZ, NP ** 3), 1.0, 6.0, ((0, 4), (1, 8)), jnp.float32)
    direction = draw_direction(jax.random.fold_in(splits[5], 71), 0)
    geometry = jnp.clip(jnp.exp(math.log(2.0) - 1.3862944 * jax.random.uniform(splits[3], (3, EA, EB, EZ, NP ** 3), jnp.float32) ** level_of(splits[3], (3, EA, EB, EZ, NP ** 3), ((1, 4), (2, 8)), -0.2, 0.2)), 0.5, 2.0).astype(jnp.bfloat16)
    mass = jnp.clip(jnp.exp(math.log(500.0) - 2.3025851 * jax.random.uniform(splits[4], (EA, EB, EZ, NP ** 3), jnp.float32) ** level_of(splits[4], (EA, EB, EZ, NP ** 3), ((0, 4), (1, 8)), -0.2, 0.2)), 50.0, 500.0).astype(jnp.bfloat16)
    return {"solution": solution, "residual": residual, "direction": direction, "geometry": geometry, "mass": mass}


lobatto_nodes = [-1.0, -0.8717401485096066, -0.5917001814331423, -0.2092992179024789,
                 0.2092992179024789, 0.5917001814331423, 0.8717401485096066, 1.0]


def derivative_table():
    nodes = np.array(lobatto_nodes)
    identity = np.eye(NP)
    offset = nodes[:, None] - nodes[None, :] + identity
    barycentric = 1.0 / np.prod(offset, axis=1)
    derivative = (barycentric[None, :] / barycentric[:, None]) / offset * (1.0 - identity)
    return derivative - identity * np.sum(derivative, axis=1)[:, None]


def operator_tables():
    derivative = derivative_table()
    identity = np.eye(NP)
    kron_list = [np.kron(np.kron(derivative, identity), identity),
                 np.kron(np.kron(identity, derivative), identity),
                 np.kron(np.kron(identity, identity), derivative)]
    forward = np.concatenate([matrix.T for matrix in kron_list], axis=1)
    backward = np.concatenate(kron_list, axis=0)
    squares = np.concatenate([matrix * matrix for matrix in kron_list], axis=0)
    return (jnp.asarray(forward, dtype=jnp.float32), jnp.asarray(backward, dtype=jnp.float32),
            jnp.asarray(squares, dtype=jnp.float32))


def point_weights():
    edge = np.where(np.arange(NP) % (NP - 1) == 0, 0.5, 1.0)
    return jnp.asarray(np.kron(np.kron(edge, edge), edge), dtype=jnp.float32)


def highest(left, right):
    return jnp.dot(left, right, precision=lax.Precision.HIGHEST, preferred_element_type=jnp.float32)


def face_pass(field, elem_dim, node_dim):
    lower = lax.index_in_dim(field, 0, node_dim, keepdims=True)
    upper = lax.index_in_dim(field, NP - 1, node_dim, keepdims=True)
    summed = upper + jnp.roll(lower, -1, axis=elem_dim)
    middle = lax.slice_in_dim(field, 1, NP - 1, axis=node_dim)
    return jnp.concatenate([jnp.roll(summed, 1, axis=elem_dim), middle, summed], axis=node_dim)


def assemble(field):
    shaped = field.reshape(field.shape[:3] + (NP, NP, NP))
    shaped = face_pass(shaped, 0, 3)
    shaped = face_pass(shaped, 1, 4)
    shaped = face_pass(shaped, 2, 5)
    return shaped.reshape(field.shape)


def reference(solution, residual, direction, geometry, mass):
    forward, backward, squares = operator_tables()
    weights = point_weights()
    points = NP ** 3
    geometry_rows = jnp.moveaxis(geometry.astype(jnp.float32), 0, -2)
    geometry_rows = geometry_rows.reshape(solution.shape[:3] + (3 * points,))
    mass_coef = mass.astype(jnp.float32)

    def diagonal_block(pair):
        geo_block, mass_block = pair
        flat = geo_block.reshape(-1, 3 * points)
        return (highest(flat, squares).reshape(mass_block.shape) + mass_block)

    def operator_block(triple):
        field_block, geo_block, mass_block = triple
        flat = field_block.reshape(-1, points)
        gradients = highest(flat, forward)
        fluxes = geo_block.reshape(-1, 3 * points) * gradients
        result = highest(fluxes, backward) + mass_block.reshape(-1, points) * flat
        return result.reshape(field_block.shape)

    diagonal = assemble(lax.map(diagonal_block, (geometry_rows, mass_coef)))
    smooth = assemble(weights * direction)
    scaled = residual / diagonal
    norm_now = jnp.sum(weights * residual * scaled)
    applied = assemble(lax.map(operator_block, (smooth, geometry_rows, mass_coef)))
    curvature = jnp.sum(weights * smooth * applied)
    step_size = norm_now / curvature
    solution_out = solution + step_size * smooth
    residual_out = residual - step_size * applied
    norm_next = jnp.sum(weights * residual_out * residual_out / diagonal)
    direction_out = residual_out / diagonal + (norm_next / norm_now) * smooth
    return (solution_out, residual_out, direction_out)
```

```python
import functools

import jax
import jax.numpy as jnp
import numpy as np
from jax import lax
from jax.experimental import pallas as pl
from jax.experimental.pallas import tpu as pltpu
from jax.sharding import PartitionSpec as P

NP = 8
LANES = 128
MESH = pl.DeviceIdType.MESH

lobatto_nodes = [
    -1.0,
    -0.8717401485096066,
    -0.5917001814331423,
    -0.2092992179024789,
    0.2092992179024789,
    0.5917001814331423,
    0.8717401485096066,
    1.0,
]


def derivative_table():
    nodes = np.array(lobatto_nodes)
    identity = np.eye(NP)
    offset = nodes[:, None] - nodes[None, :] + identity
    barycentric = 1.0 / np.prod(offset, axis=1)
    derivative = barycentric[None, :] / barycentric[:, None] / offset * (1.0 - identity)
    return derivative - identity * np.sum(derivative, axis=1)[:, None]


def split_table(table):
    table = np.asarray(table, np.float32)
    high = table.astype(jnp.bfloat16)
    low = (table - high.astype(np.float32)).astype(jnp.bfloat16)
    return high, low


def tables():
    d = derivative_table().astype(np.float32)
    along_j = np.kron(np.kron(np.eye(2), d), np.eye(NP))
    along_k = np.kron(np.eye(16), d)
    high, low = split_table(np.concatenate([along_j.T, along_k.T], axis=1))
    forward = np.concatenate([np.concatenate([high, high], 0), np.concatenate([low, low], 0)], 1)
    high, low = split_table(np.concatenate([along_j, along_k], axis=0))
    backward = np.concatenate([high, low], axis=1)
    high, low = split_table(np.concatenate([along_j * along_j, along_k * along_k], axis=0))
    squares = np.concatenate([high, low], axis=1)
    return np.concatenate([forward, backward, squares], axis=1)


def roll(x, shift):
    shift %= LANES
    return x if shift == 0 else pltpu.roll(x, shift, 1)


def lane_of(shape):
    return lax.broadcasted_iota(jnp.int32, shape, 1)


def along_i(table, blocks):
    low = lane_of(blocks[0].shape) < 64
    swapped = [roll(x, 64) for x in blocks]
    outs = []
    for b in range(4):
        total = None
        for c in range(4):
            same = jnp.where(low, float(table[2 * b, 2 * c]), float(table[2 * b + 1, 2 * c + 1]))
            other = jnp.where(low, float(table[2 * b, 2 * c + 1]), float(table[2 * b + 1, 2 * c]))
            term = same * blocks[c] + other * swapped[c]
            total = term if total is None else total + term
        outs.append(total)
    return outs


def weights_of(rows):
    lane = lane_of((rows, LANES))
    k, j = lane & 7, (lane >> 3) & 7
    half = lambda cond: jnp.where(cond, 0.5, 1.0)
    base = half((k == 0) | (k == 7)) * half((j == 0) | (j == 7))
    return [base * half(lane < 64), base, base, base * half(lane >= 64)]


def pack_i_face(x, side):
    h = x.shape[0] // 2
    top, bottom = x[:h], x[h:]
    low = lane_of(top.shape) < 64
    if side == 0:
        return jnp.where(low, top, roll(bottom, 64))
    return jnp.where(low, roll(top, 64), bottom)


def unpack_i_face(m, side):
    other = roll(m, 64)
    return jnp.concatenate([m, other] if side == 0 else [other, m], axis=0)


def pack_j_faces(fields, ez, side):
    lane = lane_of((ez, LANES))
    slot = (lane & 63) >> 3
    out = jnp.zeros((ez, LANES), jnp.float32)
    for n, blocks in enumerate(fields):
        for b in range(4):
            rows = blocks[b][:ez] if side == 0 else blocks[b][-ez:]
            moved = roll(rows, 8 * b + 32 * n - (0 if side == 0 else 56))
            out = jnp.where(slot == b + 4 * n, moved, out)
    return out


def join_j_faces(mine, before, after):
    lane = lane_of(mine.shape)
    first = (lane < 64) & ((lane & 31) < 8)
    last = (lane >= 64) & ((lane & 31) >= 24)
    return mine + jnp.where(first, roll(before, 40), jnp.where(last, roll(after, 88), 0.0))


def finish_assembly(blocks, n, ez, i_prev, i_next, j_prev, j_next):
    rows = blocks[0].shape[0]
    lane = lane_of((rows, LANES))
    low = lane < 64
    j, k = (lane >> 3) & 7, lane & 7
    blocks = list(blocks)
    blocks[0] = blocks[0] + jnp.where(low, unpack_i_face(i_prev, 0), 0.0)
    blocks[3] = blocks[3] + jnp.where(low, 0.0, unpack_i_face(i_next, 1))
    outs = []
    for b, x in enumerate(blocks):
        shift = 8 * b + 32 * n
        after, before = roll(j_next, 56 - shift), roll(j_prev, -shift)
        if rows > ez:
            after = jnp.concatenate([roll(x[ez:], 56), after], axis=0)
            before = jnp.concatenate([before, roll(x[:-ez], -56)], axis=0)
        x = x + jnp.where(j == 7, after, jnp.where(j == 0, before, 0.0))
        up, down = roll(x, 7), roll(x, -7)
        after = [pltpu.roll(up[e : e + ez], ez - 1, 0) for e in range(0, rows, ez)]
        before = [pltpu.roll(down[e : e + ez], 1, 0) for e in range(0, rows, ez)]
        after, before = jnp.concatenate(after, 0), jnp.concatenate(before, 0)
        outs.append(x + jnp.where(k == 7, after, jnp.where(k == 0, before, 0.0)))
    return outs


def halves(x):
    high = x.astype(jnp.bfloat16)
    return high, (x - high.astype(jnp.float32)).astype(jnp.bfloat16)


def dot(left, right):
    return jnp.dot(left, right, preferred_element_type=jnp.float32)


def stack(blocks):
    return jnp.concatenate(blocks, axis=0)


def total_of(blocks):
    x = blocks[0] + blocks[1] + (blocks[2] + blocks[3])
    return jnp.sum(jnp.sum(x, axis=0, keepdims=True), axis=1, keepdims=True)


def kernel(
    ng, nd, ez,
    sol_h, res_h, dir_h, geo_h, mass_h, tab_h,
    sol_o, res_o, dir_o,
    sol_v, res_v, dir_v, geo_v, mass_v, tab_v,
    i_out1, i_in1, j_out1, j_in1, i_out2, i_in2, j_out2, j_in2, part, parts,
    load_sem, send_sem, recv_sem, part_send, part_recv,
):
    me_g, me_d = lax.axis_index("group"), lax.axis_index("dev")

    def at(a, b):
        return (lax.rem(me_g + (a + ng), ng), lax.rem(me_d + (b + nd), nd))

    others = [(a, b) for a in range(ng) for b in range(nd) if (a, b) != (0, 0)]
    barrier = pltpu.get_barrier_semaphore()
    for a, b in others:
        pl.semaphore_signal(barrier, inc=1, device_id=at(a, b), device_id_type=MESH)

    pairs = ((dir_h, dir_v), (geo_h, geo_v), (mass_h, mass_v), (tab_h, tab_v), (res_h, res_v), (sol_h, sol_v))
    loads = [pltpu.make_async_copy(h, v, load_sem.at[n]) for n, (h, v) in enumerate(pairs)]
    for load in loads:
        load.start()

    rows = dir_v.shape[0]
    weights = weights_of(rows)
    cut = [slice(LANES * b, LANES * b + LANES) for b in range(4)]

    def exchange(phase, fields, i_out, i_in, j_out, j_in):
        h = rows // 2
        for n, blocks in enumerate(fields):
            i_out[0, n * h : (n + 1) * h] = pack_i_face(blocks[0], 0)
            i_out[1, n * h : (n + 1) * h] = pack_i_face(blocks[3], 1)
        for side in range(2):
            j_out[side] = pack_j_faces(fields, ez, side)
        copies = []
        for side, step in ((0, -1), (1, 1)):
            for turn, a in ((0, -1), (1, 0), (2, 1)):
                copies.append((j_out.at[side], j_in.at[side, turn], at(a, step)))
            copies.append((i_out.at[side], i_in.at[side], at(step, 0)))
        made = []
        for n, (src, dst, target) in enumerate(copies):
            made.append(
                pltpu.make_async_remote_copy(
                    src_ref=src, dst_ref=dst,
                    send_sem=send_sem.at[phase, n], recv_sem=recv_sem.at[phase, n],
                    device_id=target, device_id_type=MESH,
                )
            )
        return made

    def assembled(fields, i_in, j_in):
        h = rows // 2
        j_prev = join_j_faces(j_in[1, 1], j_in[1, 2], j_in[1, 0])
        j_next = join_j_faces(j_in[0, 1], j_in[0, 2], j_in[0, 0])
        return [
            finish_assembly(
                blocks, n, ez,
                i_in[1, n * h : (n + 1) * h], i_in[0, n * h : (n + 1) * h], j_prev, j_next,
            )
            for n, blocks in enumerate(fields)
        ]

    d = derivative_table().astype(np.float32)
    loads[0].wait()
    weighted = [weights[b] * dir_v[:, cut[b]] for b in range(4)]
    for load in loads[1:4]:
        load.wait()
    geo_rows = stack([jnp.concatenate([geo_v[1, :, c], geo_v[2, :, c]], axis=1) for c in cut])
    squared = dot(geo_rows, tab_v[:, 768:1024])
    squared = squared[:, :LANES] + squared[:, LANES:]
    geo = [[geo_v[c, :, cut[b]].astype(jnp.float32) for b in range(4)] for c in range(3)]
    mass = [mass_v[:, c].astype(jnp.float32) for c in cut]
    diag = along_i((d * d).T, geo[0])
    diag = [diag[b] + squared[rows * b : rows * b + rows] + mass[b] for b in range(4)]
    first = exchange(0, (weighted, diag), i_out1, i_in1, j_out1, j_in1)
    pl.semaphore_wait(barrier, len(others))
    for copy in first:
        copy.start()
    loads[4].wait()
    loads[5].wait()
    for copy in first:
        copy.wait_recv()
    smooth, diagonal = assembled((weighted, diag), i_in1, j_in1)

    high, low = halves(stack(smooth))
    grads = dot(jnp.concatenate([high, low], axis=1), tab_v[:, :512])
    grads = grads[:, :256] + grads[:, 256:]
    grad_i = along_i(d, smooth)
    flux_i = [geo[0][b] * grad_i[b] for b in range(4)]
    flux = jnp.concatenate(
        [stack(geo[1]) * grads[:, :LANES], stack(geo[2]) * grads[:, LANES:]], axis=1
    )
    high, low = halves(flux)
    back = dot(jnp.concatenate([high, low], axis=0), tab_v[:, 512:768])
    back = back[: 4 * rows] + back[4 * rows :]
    back = back[:, :LANES] + back[:, LANES:]
    local = along_i(d.T, flux_i)
    local = [local[b] + back[rows * b : rows * b + rows] + mass[b] * smooth[b] for b in range(4)]

    second = exchange(1, (local,), i_out2, i_in2, j_out2, j_in2)
    for copy in second:
        copy.start()
    inverse = [1.0 / x for x in diagonal]
    residual = [res_v[:, c] for c in cut]
    scaled = [residual[b] * inverse[b] for b in range(4)]
    norm_now = total_of([weights[b] * residual[b] * scaled[b] for b in range(4)])
    curvature = total_of([smooth[b] * local[b] for b in range(4)])
    for copy in second:
        copy.wait_recv()
    (applied,) = assembled((local,), i_in2, j_in2)
    shared = [weights[b] * applied[b] for b in range(4)]
    cross = total_of([shared[b] * scaled[b] for b in range(4)])
    quad = total_of([shared[b] * applied[b] * inverse[b] for b in range(4)])

    lane = lane_of((1, LANES))
    mine = jnp.where(
        lane < 32, norm_now, jnp.where(lane < 64, curvature, jnp.where(lane < 96, cross, quad))
    )
    part[0] = mine
    for n, (a, b) in enumerate(others):
        pltpu.make_async_remote_copy(
            src_ref=part.at[0], dst_ref=parts.at[n],
            send_sem=part_send, recv_sem=part_recv,
            device_id=at(a, b), device_id_type=MESH,
        ).start()
    pltpu.make_async_copy(parts, parts, part_recv).wait()
    everyone = mine + jnp.sum(parts[...], axis=0)
    norm_now, curvature, cross, quad = (everyone[:, 32 * n : 32 * n + 1] for n in range(4))
    step = norm_now / curvature
    norm_next = norm_now - 2.0 * step * cross + step * step * quad
    ratio = norm_next / norm_now
    for b, c in enumerate(cut):
        sol_o[:, c] = sol_v[:, c] + step * smooth[b]
        out = residual[b] - step * applied[b]
        res_o[:, c] = out
        dir_o[:, c] = out * inverse[b] + ratio * smooth[b]
    for copy in first + second:
        copy.wait_send()
    pltpu.make_async_copy(parts, parts, part_send).wait()


def on_device(solution, residual, direction, geometry, mass):
    dims = solution.shape
    ng, nd = lax.axis_size("group"), lax.axis_size("dev")
    ez, points = dims[2], dims[3]
    rows = dims[0] * dims[1] * ez
    flat = (rows, points)
    f32, bf16 = jnp.float32, jnp.bfloat16
    table = jnp.asarray(tables())
    h = rows // 2
    outs = pl.pallas_call(
        functools.partial(kernel, ng, nd, ez),
        out_shape=[jax.ShapeDtypeStruct(flat, f32)] * 3,
        in_specs=[pl.BlockSpec(memory_space=pl.ANY)] * 6,
        out_specs=[pl.BlockSpec(memory_space=pltpu.VMEM)] * 3,
        scratch_shapes=[
            pltpu.VMEM(flat, f32),
            pltpu.VMEM(flat, f32),
            pltpu.VMEM(flat, f32),
            pltpu.VMEM((3,) + flat, bf16),
            pltpu.VMEM(flat, bf16),
            pltpu.VMEM(table.shape, bf16),
            pltpu.VMEM((2, 2 * h, LANES), f32),
            pltpu.VMEM((2, 2 * h, LANES), f32),
            pltpu.VMEM((2, ez, LANES), f32),
            pltpu.VMEM((2, 3, ez, LANES), f32),
            pltpu.VMEM((2, h, LANES), f32),
            pltpu.VMEM((2, h, LANES), f32),
            pltpu.VMEM((2, ez, LANES), f32),
            pltpu.VMEM((2, 3, ez, LANES), f32),
            pltpu.VMEM((1, 1, LANES), f32),
            pltpu.VMEM((ng * nd - 1, 1, LANES), f32),
            pltpu.SemaphoreType.DMA((6,)),
            pltpu.SemaphoreType.DMA((2, 8)),
            pltpu.SemaphoreType.DMA((2, 8)),
            pltpu.SemaphoreType.DMA,
            pltpu.SemaphoreType.DMA,
        ],
        compiler_params=pltpu.CompilerParams(collective_id=0, has_side_effects=True),
    )(
        solution.reshape(flat),
        residual.reshape(flat),
        direction.reshape(flat),
        geometry.reshape((3,) + flat),
        mass.reshape(flat),
        table,
    )
    return tuple(x.reshape(dims) for x in outs)


def solution(mesh):
    spec = P("group", "dev", None, None)
    return jax.shard_map(
        on_device,
        mesh=mesh,
        in_specs=(spec, spec, spec, P(None, "group", "dev", None, None), spec),
        out_specs=(spec, spec, spec),
        check_vma=False,
    )
```

```python
import functools

import jax
import jax.numpy as jnp
import numpy as np
from jax import lax
from jax.experimental import pallas as pl
from jax.experimental.pallas import tpu as pltpu
from jax.sharding import PartitionSpec as P

NP = 8
LANES = 128
MESH = pl.DeviceIdType.MESH

lobatto_nodes = [
    -1.0,
    -0.8717401485096066,
    -0.5917001814331423,
    -0.2092992179024789,
    0.2092992179024789,
    0.5917001814331423,
    0.8717401485096066,
    1.0,
]


def derivative_table():
    nodes = np.array(lobatto_nodes)
    identity = np.eye(NP)
    offset = nodes[:, None] - nodes[None, :] + identity
    barycentric = 1.0 / np.prod(offset, axis=1)
    derivative = barycentric[None, :] / barycentric[:, None] / offset * (1.0 - identity)
    return derivative - identity * np.sum(derivative, axis=1)[:, None]


def split_table(table):
    table = np.asarray(table, np.float32)
    high = table.astype(jnp.bfloat16)
    low = (table - high.astype(np.float32)).astype(jnp.bfloat16)
    return high, low


def tables():
    d = derivative_table().astype(np.float32)
    along_j = np.kron(np.kron(np.eye(2), d), np.eye(NP))
    along_k = np.kron(np.eye(16), d)
    high, low = split_table(np.concatenate([along_j.T, along_k.T], axis=1))
    forward = np.concatenate([np.concatenate([high, high], 0), np.concatenate([low, low], 0)], 1)
    high, low = split_table(np.concatenate([along_j, along_k], axis=0))
    backward = np.concatenate([high, low], axis=1)
    high, low = split_table(np.concatenate([along_j * along_j, along_k * along_k], axis=0))
    squares = np.concatenate([high, low], axis=1)
    return np.concatenate([forward, backward, squares], axis=1)


def roll(x, shift):
    shift %= LANES
    return x if shift == 0 else pltpu.roll(x, shift, 1)


def lane_of(shape):
    return lax.broadcasted_iota(jnp.int32, shape, 1)


def along_i(table, blocks):
    low = lane_of(blocks[0].shape) < 64
    swapped = [roll(x, 64) for x in blocks]
    outs = []
    for b in range(4):
        total = None
        for c in range(4):
            same = jnp.where(low, float(table[2 * b, 2 * c]), float(table[2 * b + 1, 2 * c + 1]))
            other = jnp.where(low, float(table[2 * b, 2 * c + 1]), float(table[2 * b + 1, 2 * c]))
            term = same * blocks[c] + other * swapped[c]
            total = term if total is None else total + term
        outs.append(total)
    return outs


def weights_of(rows):
    lane = lane_of((rows, LANES))
    k, j = lane & 7, (lane >> 3) & 7
    half = lambda cond: jnp.where(cond, 0.5, 1.0)
    base = half((k == 0) | (k == 7)) * half((j == 0) | (j == 7))
    return [base * half(lane < 64), base, base, base * half(lane >= 64)]


def pack_i_face(x, side):
    h = x.shape[0] // 2
    top, bottom = x[:h], x[h:]
    low = lane_of(top.shape) < 64
    if side == 0:
        return jnp.where(low, top, roll(bottom, 64))
    return jnp.where(low, roll(top, 64), bottom)


def unpack_i_face(m, side):
    other = roll(m, 64)
    return jnp.concatenate([m, other] if side == 0 else [other, m], axis=0)


def pack_j_face(blocks, ez, side):
    half = ez // 2
    lane = lane_of((half, LANES))
    slot = (lane & 63) >> 3
    out = jnp.zeros((half, LANES), jnp.float32)
    for b in range(4):
        rows = blocks[b][:ez] if side == 0 else blocks[b][-ez:]
        for n in range(2):
            moved = roll(rows[n * half : (n + 1) * half], 8 * b + 32 * n - (0 if side == 0 else 56))
            out = jnp.where(slot == b + 4 * n, moved, out)
    return out


def unpack_j_face(m, b, shift):
    return jnp.concatenate([roll(m, shift - 8 * b), roll(m, shift - 8 * b - 32)], axis=0)


def join_j_faces(mine, before, after):
    lane = lane_of(mine.shape)
    first = (lane < 64) & ((lane & 31) < 8)
    last = (lane >= 64) & ((lane & 31) >= 24)
    return mine + jnp.where(first, roll(before, 40), jnp.where(last, roll(after, 88), 0.0))


def finish_assembly(blocks, ez, i_prev, i_next, j_prev, j_next):
    rows = blocks[0].shape[0]
    lane = lane_of((rows, LANES))
    low = lane < 64
    j, k = (lane >> 3) & 7, lane & 7
    blocks = list(blocks)
    blocks[0] = blocks[0] + jnp.where(low, unpack_i_face(i_prev, 0), 0.0)
    blocks[3] = blocks[3] + jnp.where(low, 0.0, unpack_i_face(i_next, 1))
    outs = []
    for b, x in enumerate(blocks):
        after, before = unpack_j_face(j_next, b, 56), unpack_j_face(j_prev, b, 0)
        if rows > ez:
            after = jnp.concatenate([roll(x[ez:], 56), after], axis=0)
            before = jnp.concatenate([before, roll(x[:-ez], -56)], axis=0)
        x = x + jnp.where(j == 7, after, jnp.where(j == 0, before, 0.0))
        up, down = roll(x, 7), roll(x, -7)
        after = [pltpu.roll(up[e : e + ez], ez - 1, 0) for e in range(0, rows, ez)]
        before = [pltpu.roll(down[e : e + ez], 1, 0) for e in range(0, rows, ez)]
        after, before = jnp.concatenate(after, 0), jnp.concatenate(before, 0)
        outs.append(x + jnp.where(k == 7, after, jnp.where(k == 0, before, 0.0)))
    return outs


def halves(x):
    high = x.astype(jnp.bfloat16)
    return high, (x - high.astype(jnp.float32)).astype(jnp.bfloat16)


def dot(left, right):
    return jnp.dot(left, right, preferred_element_type=jnp.float32)


def stack(blocks):
    return jnp.concatenate(blocks, axis=0)


def total_of(blocks):
    x = blocks[0] + blocks[1] + (blocks[2] + blocks[3])
    return jnp.sum(jnp.sum(x, axis=0, keepdims=True), axis=1, keepdims=True)


def kernel(
    ng, nd, ez,
    sol_h, res_h, dir_h, geo_h, mass_h, tab_h,
    sol_o, res_o, dir_o,
    sol_v, res_v, dir_v, geo_v, mass_v, tab_v,
    i_out, i_in, j_out, j_in, part, parts,
    load_sem, send_sem, recv_sem, part_send, part_recv,
):
    me_g, me_d = lax.axis_index("group"), lax.axis_index("dev")

    def at(a, b):
        return (lax.rem(me_g + (a + ng), ng), lax.rem(me_d + (b + nd), nd))

    others = [(a, b) for a in range(ng) for b in range(nd) if (a, b) != (0, 0)]
    barrier = pltpu.get_barrier_semaphore()
    for a, b in others:
        pl.semaphore_signal(barrier, inc=1, device_id=at(a, b), device_id_type=MESH)

    pairs = ((dir_h, dir_v), (geo_h, geo_v), (mass_h, mass_v), (tab_h, tab_v), (res_h, res_v), (sol_h, sol_v))
    loads = [pltpu.make_async_copy(h, v, load_sem.at[n]) for n, (h, v) in enumerate(pairs)]
    for load in loads:
        load.start()

    rows = dir_v.shape[0]
    weights = weights_of(rows)
    cut = [slice(LANES * b, LANES * b + LANES) for b in range(4)]

    def exchange(phase, blocks):
        copies = []
        for side, step in ((0, -1), (1, 1)):
            j_out[phase, side] = pack_j_face(blocks, ez, side)
            for turn, a in ((1, 0), (0, -1), (2, 1)):
                copies.append((j_out.at[phase, side], j_in.at[phase, side, turn], at(a, step)))
        for side, step in ((0, -1), (1, 1)):
            i_out[phase, side] = pack_i_face(blocks[3 * side], side)
            copies.append((i_out.at[phase, side], i_in.at[phase, side], at(step, 0)))
        return [
            pltpu.make_async_remote_copy(
                src_ref=src, dst_ref=dst,
                send_sem=send_sem.at[phase, n], recv_sem=recv_sem.at[phase, n],
                device_id=target, device_id_type=MESH,
            )
            for n, (src, dst, target) in enumerate(copies)
        ]

    def assembled(phase, blocks):
        j_prev = join_j_faces(j_in[phase, 1, 1], j_in[phase, 1, 2], j_in[phase, 1, 0])
        j_next = join_j_faces(j_in[phase, 0, 1], j_in[phase, 0, 2], j_in[phase, 0, 0])
        return finish_assembly(blocks, ez, i_in[phase, 1], i_in[phase, 0], j_prev, j_next)

    d = derivative_table().astype(np.float32)
    loads[0].wait()
    weighted = [weights[b] * dir_v[:, cut[b]] for b in range(4)]
    first = exchange(0, weighted)
    pl.semaphore_wait(barrier, len(others))
    for copy in first:
        copy.start()
    for load in loads[1:4]:
        load.wait()
    geo_rows = stack([jnp.concatenate([geo_v[1, :, c], geo_v[2, :, c]], axis=1) for c in cut])
    squared = dot(geo_rows, tab_v[:, 768:1024])
    squared = squared[:, :LANES] + squared[:, LANES:]
    geo = [[geo_v[c, :, cut[b]].astype(jnp.float32) for b in range(4)] for c in range(3)]
    mass = [mass_v[:, c].astype(jnp.float32) for c in cut]
    diag = along_i((d * d).T, geo[0])
    diag = [diag[b] + squared[rows * b : rows * b + rows] + mass[b] for b in range(4)]
    side_copies = exchange(1, diag)
    for copy in side_copies:
        copy.start()
    loads[4].wait()
    loads[5].wait()
    for copy in first:
        copy.wait_recv()
    smooth = assembled(0, weighted)

    high, low = halves(stack(smooth))
    grads = dot(jnp.concatenate([high, low], axis=1), tab_v[:, :512])
    grads = grads[:, :256] + grads[:, 256:]
    grad_i = along_i(d, smooth)
    flux_i = [geo[0][b] * grad_i[b] for b in range(4)]
    flux = jnp.concatenate(
        [stack(geo[1]) * grads[:, :LANES], stack(geo[2]) * grads[:, LANES:]], axis=1
    )
    high, low = halves(flux)
    back = dot(jnp.concatenate([high, low], axis=0), tab_v[:, 512:768])
    back = back[: 4 * rows] + back[4 * rows :]
    back = back[:, :LANES] + back[:, LANES:]
    local = along_i(d.T, flux_i)
    local = [local[b] + back[rows * b : rows * b + rows] + mass[b] * smooth[b] for b in range(4)]

    second = exchange(2, local)
    for copy in second:
        copy.start()
    for copy in side_copies:
        copy.wait_recv()
    inverse = [1.0 / x for x in assembled(1, diag)]
    residual = [res_v[:, c] for c in cut]
    scaled = [residual[b] * inverse[b] for b in range(4)]
    norm_now = total_of([weights[b] * residual[b] * scaled[b] for b in range(4)])
    curvature = total_of([smooth[b] * local[b] for b in range(4)])
    for copy in second:
        copy.wait_recv()
    applied = assembled(2, local)
    shared = [weights[b] * applied[b] for b in range(4)]
    cross = total_of([shared[b] * scaled[b] for b in range(4)])
    quad = total_of([shared[b] * applied[b] * inverse[b] for b in range(4)])

    lane = lane_of((1, LANES))
    mine = jnp.where(
        lane < 32, norm_now, jnp.where(lane < 64, curvature, jnp.where(lane < 96, cross, quad))
    )
    part[0] = mine
    for n, (a, b) in enumerate(others):
        pltpu.make_async_remote_copy(
            src_ref=part.at[0], dst_ref=parts.at[n],
            send_sem=part_send, recv_sem=part_recv,
            device_id=at(a, b), device_id_type=MESH,
        ).start()
    pltpu.make_async_copy(parts, parts, part_recv).wait()
    everyone = mine + jnp.sum(parts[...], axis=0)
    norm_now, curvature, cross, quad = (everyone[:, 32 * n : 32 * n + 1] for n in range(4))
    step = norm_now / curvature
    norm_next = norm_now - 2.0 * step * cross + step * step * quad
    ratio = norm_next / norm_now
    for b, c in enumerate(cut):
        sol_o[:, c] = sol_v[:, c] + step * smooth[b]
        out = residual[b] - step * applied[b]
        res_o[:, c] = out
        dir_o[:, c] = out * inverse[b] + ratio * smooth[b]
    for copy in first + side_copies + second:
        copy.wait_send()
    pltpu.make_async_copy(parts, parts, part_send).wait()


def deliver(*refs):
    copies = [pltpu.make_async_copy(refs[n], refs[3 + n], refs[6].at[n]) for n in range(3)]
    for copy in copies:
        copy.start()
    for copy in copies:
        copy.wait()


def on_device(solution, residual, direction, geometry, mass):
    dims = solution.shape
    ng, nd = lax.axis_size("group"), lax.axis_size("dev")
    ez, points = dims[2], dims[3]
    rows = dims[0] * dims[1] * ez
    flat = (rows, points)
    f32, bf16 = jnp.float32, jnp.bfloat16
    table = jnp.asarray(tables())
    h = rows // 2
    outs = pl.pallas_call(
        functools.partial(kernel, ng, nd, ez),
        out_shape=[pltpu.VMEM(flat, f32)] * 3,
        in_specs=[pl.BlockSpec(memory_space=pltpu.HBM)] * 6,
        out_specs=[pl.BlockSpec(memory_space=pltpu.VMEM)] * 3,
        scratch_shapes=[
            pltpu.VMEM(flat, f32),
            pltpu.VMEM(flat, f32),
            pltpu.VMEM(flat, f32),
            pltpu.VMEM((3,) + flat, bf16),
            pltpu.VMEM(flat, bf16),
            pltpu.VMEM(table.shape, bf16),
            pltpu.VMEM((3, 2, h, LANES), f32),
            pltpu.VMEM((3, 2, h, LANES), f32),
            pltpu.VMEM((3, 2, ez // 2, LANES), f32),
            pltpu.VMEM((3, 2, 3, ez // 2, LANES), f32),
            pltpu.VMEM((1, 1, LANES), f32),
            pltpu.VMEM((ng * nd - 1, 1, LANES), f32),
            pltpu.SemaphoreType.DMA((6,)),
            pltpu.SemaphoreType.DMA((3, 8)),
            pltpu.SemaphoreType.DMA((3, 8)),
            pltpu.SemaphoreType.DMA,
            pltpu.SemaphoreType.DMA,
        ],
        compiler_params=pltpu.CompilerParams(collective_id=0, has_side_effects=True, vmem_limit_bytes=8 << 20),
    )(
        pltpu.with_memory_space_constraint(solution.reshape(flat), pltpu.HBM),
        pltpu.with_memory_space_constraint(residual.reshape(flat), pltpu.HBM),
        pltpu.with_memory_space_constraint(direction.reshape(flat), pltpu.HBM),
        pltpu.with_memory_space_constraint(geometry.reshape((3,) + flat), pltpu.HBM),
        pltpu.with_memory_space_constraint(mass.reshape(flat), pltpu.HBM),
        pltpu.with_memory_space_constraint(table, pltpu.HBM),
    )
    outs = pl.pallas_call(
        deliver,
        out_shape=[jax.ShapeDtypeStruct(flat, f32)] * 3,
        in_specs=[pl.BlockSpec(memory_space=pl.ANY)] * 3,
        out_specs=[pl.BlockSpec(memory_space=pltpu.HBM)] * 3,
        scratch_shapes=[pltpu.SemaphoreType.DMA((3,))],
        compiler_params=pltpu.CompilerParams(vmem_limit_bytes=8 << 20),
    )(*outs)
    return tuple(x.reshape(dims) for x in outs)


def solution(mesh):
    spec = P("group", "dev", None, None)
    return jax.shard_map(
        on_device,
        mesh=mesh,
        in_specs=(spec, spec, spec, P(None, "group", "dev", None, None), spec),
        out_specs=(spec, spec, spec),
        check_vma=False,
    )
```

```python
import functools

import jax
import jax.numpy as jnp
import numpy as np
from jax import lax
from jax.experimental import pallas as pl
from jax.experimental.pallas import tpu as pltpu
from jax.sharding import PartitionSpec as P

NP = 8
LANES = 128
MESH = pl.DeviceIdType.MESH

lobatto_nodes = [
    -1.0,
    -0.8717401485096066,
    -0.5917001814331423,
    -0.2092992179024789,
    0.2092992179024789,
    0.5917001814331423,
    0.8717401485096066,
    1.0,
]


def derivative_table():
    nodes = np.array(lobatto_nodes)
    identity = np.eye(NP)
    offset = nodes[:, None] - nodes[None, :] + identity
    barycentric = 1.0 / np.prod(offset, axis=1)
    derivative = barycentric[None, :] / barycentric[:, None] / offset * (1.0 - identity)
    return derivative - identity * np.sum(derivative, axis=1)[:, None]


def split_table(table):
    table = np.asarray(table, np.float32)
    high = table.astype(jnp.bfloat16)
    low = (table - high.astype(np.float32)).astype(jnp.bfloat16)
    return high, low


def tables():
    d = derivative_table().astype(np.float32)
    along_j = np.kron(np.kron(np.eye(2), d), np.eye(NP))
    along_k = np.kron(np.eye(16), d)
    high, low = split_table(np.concatenate([along_j.T, along_k.T], axis=1))
    forward = np.concatenate([np.concatenate([high, high], 0), np.concatenate([low, low], 0)], 1)
    high, low = split_table(np.concatenate([along_j, along_k], axis=0))
    backward = np.concatenate([high, low], axis=1)
    high, low = split_table(np.concatenate([along_j * along_j, along_k * along_k], axis=0))
    squares = np.concatenate([high, low], axis=1)
    return np.concatenate([forward, backward, squares], axis=1)


def roll(x, shift):
    shift %= LANES
    return x if shift == 0 else pltpu.roll(x, shift, 1)


def lane_of(shape):
    return lax.broadcasted_iota(jnp.int32, shape, 1)


def along_i(table, blocks):
    low = lane_of(blocks[0].shape) < 64
    swapped = [roll(x, 64) for x in blocks]
    outs = []
    for b in range(4):
        total = None
        for c in range(4):
            same = jnp.where(low, float(table[2 * b, 2 * c]), float(table[2 * b + 1, 2 * c + 1]))
            other = jnp.where(low, float(table[2 * b, 2 * c + 1]), float(table[2 * b + 1, 2 * c]))
            term = same * blocks[c] + other * swapped[c]
            total = term if total is None else total + term
        outs.append(total)
    return outs


def weights_of(rows):
    lane = lane_of((rows, LANES))
    k, j = lane & 7, (lane >> 3) & 7
    half = lambda cond: jnp.where(cond, 0.5, 1.0)
    base = half((k == 0) | (k == 7)) * half((j == 0) | (j == 7))
    return [base * half(lane < 64), base, base, base * half(lane >= 64)]


def pack_i_face(x, side):
    h = x.shape[0] // 2
    top, bottom = x[:h], x[h:]
    low = lane_of(top.shape) < 64
    if side == 0:
        return jnp.where(low, top, roll(bottom, 64))
    return jnp.where(low, roll(top, 64), bottom)


def unpack_i_face(m, side):
    other = roll(m, 64)
    return jnp.concatenate([m, other] if side == 0 else [other, m], axis=0)


def pack_j_face(blocks, ez, side):
    half = ez // 2
    lane = lane_of((half, LANES))
    slot = (lane & 63) >> 3
    out = jnp.zeros((half, LANES), jnp.float32)
    for b in range(4):
        rows = blocks[b][:ez] if side == 0 else blocks[b][-ez:]
        for n in range(2):
            moved = roll(rows[n * half : (n + 1) * half], 8 * b + 32 * n - (0 if side == 0 else 56))
            out = jnp.where(slot == b + 4 * n, moved, out)
    return out


def unpack_j_face(m, b, shift):
    return jnp.concatenate([roll(m, shift - 8 * b), roll(m, shift - 8 * b - 32)], axis=0)


def join_j_faces(mine, before, after):
    lane = lane_of(mine.shape)
    first = (lane < 64) & ((lane & 31) < 8)
    last = (lane >= 64) & ((lane & 31) >= 24)
    return mine + jnp.where(first, roll(before, 40), jnp.where(last, roll(after, 88), 0.0))


def finish_assembly(blocks, ez, i_prev, i_next, j_prev, j_next):
    rows = blocks[0].shape[0]
    lane = lane_of((rows, LANES))
    low = lane < 64
    j, k = (lane >> 3) & 7, lane & 7
    blocks = list(blocks)
    blocks[0] = blocks[0] + jnp.where(low, unpack_i_face(i_prev, 0), 0.0)
    blocks[3] = blocks[3] + jnp.where(low, 0.0, unpack_i_face(i_next, 1))
    outs = []
    for b, x in enumerate(blocks):
        after, before = unpack_j_face(j_next, b, 56), unpack_j_face(j_prev, b, 0)
        if rows > ez:
            after = jnp.concatenate([roll(x[ez:], 56), after], axis=0)
            before = jnp.concatenate([before, roll(x[:-ez], -56)], axis=0)
        x = x + jnp.where(j == 7, after, jnp.where(j == 0, before, 0.0))
        up, down = roll(x, 7), roll(x, -7)
        after = [pltpu.roll(up[e : e + ez], ez - 1, 0) for e in range(0, rows, ez)]
        before = [pltpu.roll(down[e : e + ez], 1, 0) for e in range(0, rows, ez)]
        after, before = jnp.concatenate(after, 0), jnp.concatenate(before, 0)
        outs.append(x + jnp.where(k == 7, after, jnp.where(k == 0, before, 0.0)))
    return outs


def halves(x):
    high = x.astype(jnp.bfloat16)
    return high, (x - high.astype(jnp.float32)).astype(jnp.bfloat16)


def dot(left, right):
    return jnp.dot(left, right, preferred_element_type=jnp.float32)


def stack(blocks):
    return jnp.concatenate(blocks, axis=0)


def total_of(blocks):
    x = blocks[0] + blocks[1] + (blocks[2] + blocks[3])
    return jnp.sum(jnp.sum(x, axis=0, keepdims=True), axis=1, keepdims=True)


def kernel(
    ng, nd, ez,
    sol_h, res_h, dir_h, geo_h, mass_h, tab_h,
    sol_o, res_o, dir_o,
    sol_v, res_v, dir_v, geo_v, mass_v, tab_v,
    i_out, i_in, j_out, j_in, part, parts,
    load_sem, send_sem, recv_sem, part_send, part_recv,
):
    me_g, me_d = lax.axis_index("group"), lax.axis_index("dev")

    def at(a, b):
        return (lax.rem(me_g + (a + ng), ng), lax.rem(me_d + (b + nd), nd))

    others = [(a, b) for a in range(ng) for b in range(nd) if (a, b) != (0, 0)]
    others.sort(key=lambda t: (min(t[1], nd - t[1]) != 1, min(t[0], ng - t[0]) > 1))
    barrier = pltpu.get_barrier_semaphore()
    for a, b in others:
        pl.semaphore_signal(barrier, inc=1, device_id=at(a, b), device_id_type=MESH)

    pairs = ((dir_h, dir_v), (geo_h, geo_v), (mass_h, mass_v), (tab_h, tab_v), (res_h, res_v), (sol_h, sol_v))
    loads = [pltpu.make_async_copy(h, v, load_sem.at[n]) for n, (h, v) in enumerate(pairs)]
    for load in loads:
        load.start()

    rows = dir_v.shape[0]
    weights = weights_of(rows)
    cut = [slice(LANES * b, LANES * b + LANES) for b in range(4)]

    def exchange(phase, blocks, started=True):
        made = []

        def give(src, dst, target):
            n = len(made)
            made.append(
                pltpu.make_async_remote_copy(
                    src_ref=src, dst_ref=dst,
                    send_sem=send_sem.at[phase, n], recv_sem=recv_sem.at[phase, n],
                    device_id=target, device_id_type=MESH,
                )
            )
            if started:
                made[-1].start()

        for side, step in ((0, -1), (1, 1)):
            i_out[phase, side] = pack_i_face(blocks[3 * side], side)
            give(i_out.at[phase, side], i_in.at[phase, side], at(step, 0))
        for side, step in ((1, 1), (0, -1)):
            j_out[phase, side] = pack_j_face(blocks, ez, side)
            for turn, a in ((0, -1), (2, 1), (1, 0)):
                give(j_out.at[phase, side], j_in.at[phase, side, turn], at(a, step))
        return made

    def assembled(phase, blocks):
        j_prev = join_j_faces(j_in[phase, 1, 1], j_in[phase, 1, 2], j_in[phase, 1, 0])
        j_next = join_j_faces(j_in[phase, 0, 1], j_in[phase, 0, 2], j_in[phase, 0, 0])
        return finish_assembly(blocks, ez, i_in[phase, 1], i_in[phase, 0], j_prev, j_next)

    d = derivative_table().astype(np.float32)
    loads[0].wait()
    weighted = [weights[b] * dir_v[:, cut[b]] for b in range(4)]
    first = exchange(0, weighted, started=False)
    pl.semaphore_wait(barrier, len(others))
    for copy in first:
        copy.start()
    for load in loads[1:4]:
        load.wait()
    geo_rows = stack([jnp.concatenate([geo_v[1, :, c], geo_v[2, :, c]], axis=1) for c in cut])
    squared = dot(geo_rows, tab_v[:, 768:1024])
    squared = squared[:, :LANES] + squared[:, LANES:]
    geo = [[geo_v[c, :, cut[b]].astype(jnp.float32) for b in range(4)] for c in range(3)]
    mass = [mass_v[:, c].astype(jnp.float32) for c in cut]
    diag = along_i((d * d).T, geo[0])
    diag = [diag[b] + squared[rows * b : rows * b + rows] + mass[b] for b in range(4)]
    side_copies = exchange(1, diag)
    loads[4].wait()
    loads[5].wait()
    for copy in first:
        copy.wait_recv()
    smooth = assembled(0, weighted)

    high, low = halves(stack(smooth))
    grads = dot(jnp.concatenate([high, low], axis=1), tab_v[:, :512])
    grads = grads[:, :256] + grads[:, 256:]
    grad_i = along_i(d, smooth)
    flux_i = [geo[0][b] * grad_i[b] for b in range(4)]
    flux = jnp.concatenate(
        [stack(geo[1]) * grads[:, :LANES], stack(geo[2]) * grads[:, LANES:]], axis=1
    )
    high, low = halves(flux)
    back = dot(jnp.concatenate([high, low], axis=0), tab_v[:, 512:768])
    back = back[: 4 * rows] + back[4 * rows :]
    back = back[:, :LANES] + back[:, LANES:]
    local = along_i(d.T, flux_i)
    local = [local[b] + back[rows * b : rows * b + rows] + mass[b] * smooth[b] for b in range(4)]

    second = exchange(2, local)
    for copy in side_copies:
        copy.wait_recv()
    inverse = [1.0 / x for x in assembled(1, diag)]
    residual = [res_v[:, c] for c in cut]
    scaled = [residual[b] * inverse[b] for b in range(4)]
    norm_now = total_of([weights[b] * residual[b] * scaled[b] for b in range(4)])
    curvature = total_of([smooth[b] * local[b] for b in range(4)])
    for copy in second:
        copy.wait_recv()
    applied = assembled(2, local)
    shared = [weights[b] * applied[b] for b in range(4)]
    cross = total_of([shared[b] * scaled[b] for b in range(4)])
    quad = total_of([shared[b] * applied[b] * inverse[b] for b in range(4)])

    lane = lane_of((1, LANES))
    mine = jnp.where(
        lane < 32, norm_now, jnp.where(lane < 64, curvature, jnp.where(lane < 96, cross, quad))
    )
    part[0] = mine
    for n, (a, b) in enumerate(others):
        pltpu.make_async_remote_copy(
            src_ref=part.at[0], dst_ref=parts.at[n],
            send_sem=part_send, recv_sem=part_recv,
            device_id=at(a, b), device_id_type=MESH,
        ).start()
    pltpu.make_async_copy(parts, parts, part_recv).wait()
    everyone = mine + jnp.sum(parts[...], axis=0)
    norm_now, curvature, cross, quad = (everyone[:, 32 * n : 32 * n + 1] for n in range(4))
    step = norm_now / curvature
    norm_next = norm_now - 2.0 * step * cross + step * step * quad
    ratio = norm_next / norm_now
    for b, c in enumerate(cut):
        sol_o[:, c] = sol_v[:, c] + step * smooth[b]
        out = residual[b] - step * applied[b]
        res_o[:, c] = out
        dir_o[:, c] = out * inverse[b] + ratio * smooth[b]
    for copy in first + side_copies + second:
        copy.wait_send()
    pltpu.make_async_copy(parts, parts, part_send).wait()


def deliver(*refs):
    copies = [pltpu.make_async_copy(refs[n], refs[3 + n], refs[6].at[n]) for n in range(3)]
    for copy in copies:
        copy.start()
    for copy in copies:
        copy.wait()


def on_device(solution, residual, direction, geometry, mass):
    dims = solution.shape
    ng, nd = lax.axis_size("group"), lax.axis_size("dev")
    ez, points = dims[2], dims[3]
    rows = dims[0] * dims[1] * ez
    flat = (rows, points)
    f32, bf16 = jnp.float32, jnp.bfloat16
    table = jnp.asarray(tables())
    h = rows // 2
    outs = pl.pallas_call(
        functools.partial(kernel, ng, nd, ez),
        out_shape=[pltpu.VMEM(flat, f32)] * 3,
        in_specs=[pl.BlockSpec(memory_space=pltpu.HBM)] * 6,
        out_specs=[pl.BlockSpec(memory_space=pltpu.VMEM)] * 3,
        scratch_shapes=[
            pltpu.VMEM(flat, f32),
            pltpu.VMEM(flat, f32),
            pltpu.VMEM(flat, f32),
            pltpu.VMEM((3,) + flat, bf16),
            pltpu.VMEM(flat, bf16),
            pltpu.VMEM(table.shape, bf16),
            pltpu.VMEM((3, 2, h, LANES), f32),
            pltpu.VMEM((3, 2, h, LANES), f32),
            pltpu.VMEM((3, 2, ez // 2, LANES), f32),
            pltpu.VMEM((3, 2, 3, ez // 2, LANES), f32),
            pltpu.VMEM((1, 1, LANES), f32),
            pltpu.VMEM((ng * nd - 1, 1, LANES), f32),
            pltpu.SemaphoreType.DMA((6,)),
            pltpu.SemaphoreType.DMA((3, 8)),
            pltpu.SemaphoreType.DMA((3, 8)),
            pltpu.SemaphoreType.DMA,
            pltpu.SemaphoreType.DMA,
        ],
        compiler_params=pltpu.CompilerParams(collective_id=0, has_side_effects=True, vmem_limit_bytes=8 << 20),
    )(
        pltpu.with_memory_space_constraint(solution.reshape(flat), pltpu.HBM),
        pltpu.with_memory_space_constraint(residual.reshape(flat), pltpu.HBM),
        pltpu.with_memory_space_constraint(direction.reshape(flat), pltpu.HBM),
        pltpu.with_memory_space_constraint(geometry.reshape((3,) + flat), pltpu.HBM),
        pltpu.with_memory_space_constraint(mass.reshape(flat), pltpu.HBM),
        pltpu.with_memory_space_constraint(table, pltpu.HBM),
    )
    outs = pl.pallas_call(
        deliver,
        out_shape=[jax.ShapeDtypeStruct(flat, f32)] * 3,
        in_specs=[pl.BlockSpec(memory_space=pl.ANY)] * 3,
        out_specs=[pl.BlockSpec(memory_space=pltpu.HBM)] * 3,
        scratch_shapes=[pltpu.SemaphoreType.DMA((3,))],
        compiler_params=pltpu.CompilerParams(vmem_limit_bytes=8 << 20),
    )(*outs)
    return tuple(x.reshape(dims) for x in outs)


def solution(mesh):
    spec = P("group", "dev", None, None)
    return jax.shard_map(
        on_device,
        mesh=mesh,
        in_specs=(spec, spec, spec, P(None, "group", "dev", None, None), spec),
        out_specs=(spec, spec, spec),
        check_vma=False,
    )
```
